32 devices in a mesh: groups: 2 (over y), expert: 4 (over x, core), tensor: 4 (over z).
Axes of the slice: x: 2, y: 2, z: 4, core: 2. Of those that a mesh axis runs over, the one named last changes fastest.
Arguments:
- tokens: bfloat16 [512, 4096], P(('groups', 'expert'), 'tensor'), parts along dimension 0, may hold values from -400 to 400
- norm_gain: float32 [4096], replicated, may hold values from 0.5 to 1.5
- w_gate: bfloat16 [4096, 65536], P(None, ('expert', 'tensor')), may hold values from -0.09375 to 0.09375
- w_up: bfloat16 [4096, 65536], P(None, ('expert', 'tensor')), may hold values from -0.09375 to 0.09375
- w_down: bfloat16 [65536, 4096], P(('expert', 'tensor')), may hold values from -0.0625 to 0.0625
- expert_ids: int32 [512, 2], P(('groups', 'expert')), parts along dimension 0, may hold values from 0 to 7, all different within a row; in each aligned block of 64 rows (0 to 63, 64 to 127, ...) at most 32 rows name the same one
- gate_weights: float32 [512, 2], P(('groups', 'expert')), parts along dimension 0, may hold values from 0.1 to 1
Outputs:
- moe_out: bfloat16 [512, 4096], P(('groups', 'expert'), 'tensor'), parts along dimension 0
The draws below stay inside these ranges and needn't reach their ends.
There are 2 independent parts, one for each index of `groups`. The reference program is written for one: setup_inputs(seed, part) draws one part's arguments, and reference() takes and returns one part's arrays. A program takes and returns all parts, laid end to end along the dimension named above; an argument that names none is the same for every part. Nothing has to cross between parts.
Inputs may be any that keep to these rules, and one draw needn't show every extreme that they name: `expert_ids`: each request names two different experts. Within the rows of one device (aligned blocks of 64 rows) no expert is named by more than 32 rows, and in some blocks one expert is named by exactly 32 rows.
All inputs are finite; a program needn't handle non-finite values.
Results may differ from the reference program's by a relative error of at most 0.008.
Values may be sent and summed in bfloat16 or wider, within the bound.
A program may use at most 192 MiB of HBM per device.

```python
import math
import jax
import jax.numpy as jnp
import numpy as np
from jax import lax

WIDTH = 4096
EXPERT_HIDDEN = 8192
EXPERTS = 8
TOK_DEV = 64
SLOTS = 32
TOKENS = 256
N_EXPERT = 4


def draw_tokens(key, part):
    key_base, key_rows, key_cols = jax.random.split(key, 3)
    row_scale = jnp.exp(jax.random.uniform(key_rows, (TOKENS, 1), jnp.float32, 0.0, 2.3))
    ramp = jnp.exp(jnp.log(3.0) * jnp.arange(WIDTH, dtype=jnp.float32) / WIDTH)
    col_scale = ramp[None, :] * jnp.exp(jax.random.uniform(key_cols, (1, WIDTH), jnp.float32, -1.15, 1.15))
    base = jax.random.truncated_normal(key_base, -4.0, 4.0, (TOKENS, WIDTH), jnp.float32)
    return jnp.clip(base * row_scale * col_scale, -400.0, 400.0).astype(jnp.bfloat16)


def level_of(own_key, shape, shards, least, largest):
    gain, own = 1.0, jax.random.fold_in(own_key, 6)
    for dim, blocks in shards:
        draws = jnp.exp(jax.random.uniform(jax.random.fold_in(own, dim), (blocks,), jnp.float32, least / len(shards), largest / len(shards)))
        gain = gain * jnp.repeat(draws, shape[dim] // blocks).reshape([-1 if axis == dim else 1 for axis in range(len(shape))])
    return gain


def shared_out(stream_key, own, number, rows, amount, top, most, skew):
    sequence = jax.random.permutation(stream_key, amount)
    packed, usual = shares(amount, rows * top, most, skew, True), shares(amount, rows * top, most, skew, False)
    places = jnp.arange(amount)

    def named(sizes, turn):
        used = int((sizes > 0).sum())
        fixed = max(1, used // 4)
        shifted = fixed + (places - fixed + turn * (used - fixed)) % max(1, amount - fixed)
        return jnp.zeros((amount,), jnp.int32).at[sequence[jnp.where(places < fixed, places, shifted)]].set(jnp.asarray(sizes, jnp.int32))

    sizes = jnp.where(number % 4 == 0, named(packed, number // 4), named(usual, number - number // 4 - 1))
    mixed = jax.random.permutation(jax.random.fold_in(own, 3), amount)
    donor, receiver = mixed[0:amount // 2 * 2:2], mixed[1:amount // 2 * 2:2]
    room = jnp.minimum(sizes[donor] - 1, most - sizes[receiver]) // 2
    room = jnp.where((donor == sequence[0]) | (receiver == sequence[0]) | (sizes[receiver] == 0), 0, jnp.maximum(room, 0))
    shifted = jax.random.randint(jax.random.fold_in(own, 4), (amount // 2,), 0, 1 << 20) % (room + 1)
    sizes = sizes.at[donor].add(-shifted).at[receiver].add(shifted)
    members = jnp.searchsorted(jnp.cumsum(sizes), jnp.arange(rows * top), side="right").astype(jnp.int32)
    grid = members.reshape(top, rows).T
    grid = grid[jax.random.permutation(jax.random.fold_in(own, 1), rows)]
    turn = jax.random.randint(jax.random.fold_in(own, 2), (rows, 1), 0, top)
    return jnp.take_along_axis(grid, (jnp.arange(top)[None, :] + turn) % top, axis=1)


def shares(number_of, total, most, skew, full):
    weights = [(1 << 20) // math.isqrt(rank ** skew) + 1 for rank in range(1, number_of + 1)]
    largest = most if full else min(most, max(-(-total // number_of), total * weights[0] // sum(weights)))
    least = 1 if total - largest >= number_of - 1 else 0
    given, surplus = [largest] + [least] * (number_of - 1), total - largest - least * (number_of - 1)
    while surplus > 0:
        free = [i for i in range(1, number_of) if given[i] < largest] or [i for i in range(1, number_of) if given[i] < most]
        whole, remaining = sum([weights[i] for i in free]), surplus
        for i in free:
            more = min(most - given[i], max(1, remaining * weights[i] // whole), surplus)
            given[i] = given[i] + more
            surplus = surplus - more
    return np.array(given)


def scatter_about(stream_key, extent, deviation, reach, cuts=(), held_as=jnp.bfloat16):
    level = level_of(stream_key, extent, cuts, -0.22, 0.18) if cuts else 1.0
    values = jax.random.normal(stream_key, extent, jnp.float32) * deviation * level
    return jnp.minimum(jnp.maximum(values, -reach), reach).astype(held_as)


def setup_inputs(seed: int = 0, part: int = 0) -> dict:
    splits = jax.random.split(jax.random.key(seed), 8)
    part_splits = jax.random.split(jax.random.fold_in(splits[7], part), 8)
    tokens = draw_tokens(jax.random.fold_in(jax.random.fold_in(splits[7], part), 71), part)
    norm_gain = jnp.clip(1.0 + 0.1 * jax.random.normal(splits[1], (WIDTH,), jnp.float32), 0.5, 1.5)
    w_gate = scatter_about(splits[2], (WIDTH, EXPERTS * EXPERT_HIDDEN), WIDTH ** -0.5, 0.09375, ((1, 16),))
    w_up = scatter_about(splits[3], (WIDTH, EXPERTS * EXPERT_HIDDEN), WIDTH ** -0.5, 0.09375, ((1, 16),))
    w_down = scatter_about(splits[4], (EXPERTS * EXPERT_HIDDEN, WIDTH), EXPERT_HIDDEN ** -0.5, 0.0625, ((0, 16),))
    expert_ids_keys = jax.random.split(jax.random.fold_in(part_splits[5], 1), TOKENS // TOK_DEV)
    expert_ids_turns = jax.random.permutation(jax.random.fold_in(part_splits[5], 3), TOKENS // TOK_DEV)
    expert_ids = jax.vmap(lambda own, number: shared_out(jax.random.fold_in(part_splits[5], 2), own, number, TOK_DEV, EXPERTS, 2, SLOTS, 2))(expert_ids_keys, expert_ids_turns).reshape((TOKENS, 2))
    gate_weights = jnp.clip(0.1 + 0.9 * jax.random.uniform(part_splits[6], (TOKENS, 2), jnp.float32) ** level_of(part_splits[6], (TOKENS, 2), ((0, 4),), -0.2, 0.2), 0.1, 1.0)
    return {"tokens": tokens, "norm_gain": norm_gain, "w_gate": w_gate, "w_up": w_up, "w_down": w_down, "expert_ids": expert_ids, "gate_weights": gate_weights}


def reference(tokens, norm_gain, w_gate, w_up, w_down, expert_ids, gate_weights):
    values = tokens.astype(jnp.float32)
    mean_square = lax.optimization_barrier(jnp.mean(values * values, axis=1, keepdims=True))
    normed = (values * lax.rsqrt(mean_square + 1e-05) * norm_gain[None, :]).astype(jnp.bfloat16)
    capacity_all = N_EXPERT * SLOTS
    result = jnp.zeros((TOKENS, WIDTH), jnp.float32)
    for expert in range(EXPERTS):
        chosen = expert_ids == expert
        weight_of = lax.optimization_barrier(jnp.sum(jnp.where(chosen, gate_weights, jnp.zeros_like(gate_weights)), axis=1))
        is_routed = jnp.any(chosen, axis=1).astype(jnp.int32)
        picked = jnp.argsort(1 - is_routed, stable=True)[:capacity_all].astype(jnp.int32)
        row_data = jnp.take(normed, picked, axis=0)
        low = expert * EXPERT_HIDDEN
        high = low + EXPERT_HIDDEN
        gate_act = jnp.dot(row_data, w_gate[:, low:high], preferred_element_type=jnp.float32)
        up_act = jnp.dot(row_data, w_up[:, low:high], preferred_element_type=jnp.float32)
        hidden = (jax.nn.silu(gate_act) * up_act).astype(jnp.bfloat16)
        expert_out = jnp.dot(hidden, w_down[low:high, :], preferred_element_type=jnp.float32)
        weights_here = jnp.take(weight_of, picked, axis=0)
        result = result.at[picked].add(weights_here[:, None] * expert_out)
    return result.astype(jnp.bfloat16)
```

```python
import functools

import jax
import jax.numpy as jnp
from jax import lax
from jax.experimental import pallas as pl
from jax.experimental.pallas import tpu as pltpu
from jax.sharding import PartitionSpec as P

EXPERTS = 8
MIB = 1 << 20
MESH = pl.DeviceIdType.MESH
LANES = 128


def kernel(
    n_e, n_t, cap, ring, lag, pieces, dc,
    tokens, gain_in, ids_in, weights_in, w_gate, w_up, w_down,
    out,
    wbuf, blocks, gain, ids, weights, spread, place, wsend, wslot, sendpk, recvpk, packed, ssq, scale,
    acc_gate, acc_up, hidden,
    sendbuf, recvbuf, zsend, zrecv, outbuf,
    wsem, lsem, rsem, zsem, psend, precv, msend, mrecv, osend, orecv, ysend, yrecv,
):
    g, e, t = lax.axis_index("groups"), lax.axis_index("expert"), lax.axis_index("tensor")
    rows, kr = tokens.shape
    width = w_gate.shape[0]
    hid = w_gate.shape[1]
    sc = wbuf.shape[2]
    slots = n_e * cap
    per_expert = n_e * n_t // EXPERTS
    nj = hid // sc
    gate_units = n_t * nj
    parts = hid // kr
    per_slot = sc // dc
    per_slice = kr // dc
    down_chunks = n_t * per_slice
    units = gate_units + down_chunks
    kp = kr // pieces

    def order(s):
        return jnp.bitwise_xor(t, s)

    def slice_of(k):
        return order(2 * lax.rem(k // 2 + 1, n_t // 2) + 1 - lax.rem(k, 2))

    def columns(start, size):
        return pl.ds(pl.multiple_of(start, size), size)

    def down_columns(d):
        return columns(slice_of(d // per_slice) * kr + (d % per_slice) * dc, dc)

    def gate_copies(u, q, j):
        slot = lax.rem(u, ring) * 2
        at = (columns(q * kr, kr), columns(j * sc, sc))
        return (
            pltpu.make_async_copy(w_gate.at[at], wbuf.at[slot], wsem.at[slot, 0]),
            pltpu.make_async_copy(w_up.at[at], wbuf.at[slot + 1], wsem.at[slot + 1, 0]),
        )

    def down_copies(d):
        slot = lax.rem(gate_units + d, ring) * 2
        return [
            pltpu.make_async_copy(
                w_down.at[k * kr:(k + 1) * kr, down_columns(d)],
                wbuf.at[slot + k // per_slot, :, k % per_slot * dc:(k % per_slot + 1) * dc],
                wsem.at[slot + k // per_slot, k % per_slot],
            )
            for k in range(parts)
        ]

    def start_unit(u):
        @pl.when(u < gate_units)
        def _():
            for copy in gate_copies(u, order(u // nj), u % nj):
                copy.start()

        @pl.when(jnp.logical_and(u >= gate_units, u < units))
        def _():
            for copy in down_copies(u - gate_units):
                copy.start()

    def block_copy(q, p, send_sem, to):
        return pltpu.make_async_remote_copy(
            src_ref=blocks.at[q, p], dst_ref=blocks.at[q, p],
            send_sem=send_sem, recv_sem=rsem.at[q, p], device_id=(g, e, to), device_id_type=MESH,
        )

    def z_copy(j, p):
        return block_copy(t, p, zsem.at[j, p], order(j))

    def z_relay(s, p):
        return block_copy(order(s), p, zsem.at[s + 1, p], order(1))

    def rows_copy(src, dst, send_sem, recv_sem, o):
        ej = lax.rem(e + o, n_e)
        return pltpu.make_async_remote_copy(
            src_ref=src.at[columns(ej * cap, cap)], dst_ref=dst.at[columns(e * cap, cap)],
            send_sem=send_sem, recv_sem=recv_sem.at[e], device_id=(g, ej, t), device_id_type=MESH,
        )

    def rows_arrived(src, dst, send_sem, recv_sem, o):
        ej = lax.rem(e + o, n_e)
        at = columns(ej * cap, cap)
        pltpu.make_async_remote_copy(
            src_ref=src.at[at], dst_ref=dst.at[at],
            send_sem=send_sem, recv_sem=recv_sem.at[ej], device_id=(g, ej, t), device_id_type=MESH,
        ).wait_recv()

    def p_copy(o, q, p):
        return rows_copy(sendpk.at[q, p], recvpk.at[q, p], psend.at[o, q, p], precv.at[q, p], o)

    def m_copy(o):
        return rows_copy(wsend, wslot, msend.at[o], mrecv, o)

    own_rows = columns(e * cap, cap)

    local = [
        pltpu.make_async_copy(ids_in, ids, lsem.at[0]),
        pltpu.make_async_copy(weights_in, weights, lsem.at[1]),
        pltpu.make_async_copy(gain_in, gain, lsem.at[2]),
    ] + [
        pltpu.make_async_copy(tokens.at[:, p * kp:(p + 1) * kp], blocks.at[t, p], lsem.at[3 + p])
        for p in range(pieces)
    ]
    for copy in local:
        copy.start()
    barrier = pltpu.get_barrier_semaphore()
    for o in range(1, n_e):
        pl.semaphore_signal(barrier, inc=1, device_id=(g, lax.rem(e + o, n_e), t), device_id_type=MESH)
    for o in range(1, n_t):
        pl.semaphore_signal(barrier, inc=1, device_id=(g, e, lax.rem(t + o, n_t)), device_id_type=MESH)

    def prefetch(u, _):
        start_unit(u)
        return 0

    lax.fori_loop(0, min(ring, units), prefetch, 0)
    for copy in local:
        copy.wait()

    upper = (
        lax.broadcasted_iota(jnp.int32, (rows, rows), 0) < lax.broadcasted_iota(jnp.int32, (rows, rows), 1)
    ).astype(jnp.float32).astype(jnp.bfloat16)

    for ej in range(n_e):
        expert = (ej * n_t + t) // per_expert
        named = jnp.where(ids[0:1, :] == expert, 1.0, 0.0) + jnp.where(ids[1:2, :] == expert, 1.0, 0.0)
        rank = jnp.dot(
            jnp.broadcast_to(named, (8, rows)).astype(jnp.bfloat16), upper, preferred_element_type=jnp.float32
        )[0:1, :]
        slot = lax.broadcasted_iota(jnp.int32, (cap, rows), 0).astype(jnp.float32)
        hit = jnp.where(slot == rank, 1.0, 0.0) * named
        weight = jnp.where(ids[0:1, :] == expert, weights[0:1, :], weights[1:2, :])
        at = slice(ej * cap, (ej + 1) * cap)
        spread[at, :] = hit.astype(jnp.bfloat16)
        wsend[at, :] = jnp.broadcast_to(jnp.sum(hit * weight, axis=1, keepdims=True), (cap, LANES))
        filled = jnp.concatenate([hit, jnp.zeros((cap, LANES - rows), jnp.float32)], axis=1)
        place[:, at] = jnp.transpose(filled)[0:rows, :].astype(jnp.bfloat16)
    wslot[own_rows, :] = wsend[own_rows, :]
    ssq[...] = jnp.zeros_like(ssq)

    pl.semaphore_wait(barrier, n_e - 1 + n_t - 1)

    def dispatch(q, p):
        picked = jnp.dot(spread[...], blocks[q, p], preferred_element_type=jnp.float32)
        sendpk[q, p] = picked.astype(jnp.bfloat16)
        for o in range(1, n_e):
            p_copy(o, q, p).start()
        recvpk[q, p, own_rows, :] = sendpk[q, p, own_rows, :]

    def take(s):
        q = order(s)
        for p in range(pieces):
            block_copy(q, p, zsem.at[1, 0], order(1)).wait_recv()

            @pl.when(lax.rem(s, 2) == 0)
            def _():
                z_relay(s, p).start()

            dispatch(q, p)

    def pack(q):
        for p in range(pieces):
            for o in range(1, n_e):
                rows_arrived(sendpk.at[q, p], recvpk.at[q, p], psend.at[0, 0, 0], precv.at[q, p], o)
            gain_q = gain[:, columns(q * kr + p * kp, kp)]
            for r in range(slots // 32):
                at = slice(r * 32, (r + 1) * 32)
                value = recvpk[q, p, at, :].astype(jnp.float32)
                square = value * value
                total = square[:, 0:LANES]
                for c in range(1, kp // LANES):
                    total += square[:, c * LANES:(c + 1) * LANES]
                ssq[at, :] += total
                packed[p, at, :] = (value * gain_q).astype(jnp.bfloat16)

    def contract(ref, inner):
        value = jnp.dot(packed[0], ref[0:kp, inner], preferred_element_type=jnp.float32)
        for p in range(1, pieces):
            value += jnp.dot(packed[p], ref[p * kp:(p + 1) * kp, inner], preferred_element_type=jnp.float32)
        return value

    def expert_in(s, first, last):
        q = order(s)
        pack(q)
        if last:
            mean = jnp.sum(ssq[...], axis=1, keepdims=True) / width
            scale[...] = jnp.broadcast_to(lax.rsqrt(mean + 1e-05), scale.shape)

        def one(j, _):
            u = s * nj + j
            slot = lax.rem(u, ring) * 2
            if not last:
                @pl.when(j == nj // 2)
                def _():
                    @pl.when(s + 2 < n_t)
                    def _():
                        take(s + 2)

            for copy in gate_copies(u, q, j):
                copy.wait()
            wide = min(512, sc)
            for n in range(sc // wide):
                inner = slice(n * wide, (n + 1) * wide)
                at = columns(j * sc + n * wide, wide)
                gate = contract(wbuf.at[slot], inner)
                if not first:
                    gate += acc_gate[:, at]
                up = contract(wbuf.at[slot + 1], inner)
                if not first:
                    up += acc_up[:, at]
                if last:
                    for c in range(wide // LANES):
                        lanes = slice(c * LANES, (c + 1) * LANES)
                        gated = gate[:, lanes] * scale[...]
                        value = gated / (1.0 + jnp.exp(-gated)) * (up[:, lanes] * scale[...])
                        hidden[:, columns(j * sc + n * wide + c * LANES, LANES)] = value.astype(jnp.bfloat16)
                else:
                    acc_gate[:, at] = gate
                    acc_up[:, at] = up
            start_unit(u + ring)
            return 0

        lax.fori_loop(0, nj, one, 0)

    for p in range(pieces):
        z_copy(1, p).start()
    for j in range(2, n_t, 2):
        for p in range(pieces):
            z_copy(j, p).start()
    for p in range(pieces):
        dispatch(t, p)
    take(jnp.int32(1))
    expert_in(jnp.int32(0), True, False)

    def middle(s, _):
        expert_in(s, False, False)
        return 0

    lax.fori_loop(1, n_t - 1, middle, 0)
    for o in range(1, n_e):
        m_copy(o).start()
    expert_in(jnp.int32(n_t - 1), False, True)

    for o in range(1, n_e):
        rows_arrived(wsend, wslot, msend.at[0], mrecv, o)

    def o_copy(o, d):
        return rows_copy(sendbuf.at[d], recvbuf.at[d], osend.at[o, d], orecv.at[d], o)

    def o_arrived(o, d):
        rows_arrived(sendbuf.at[d], recvbuf.at[d], osend.at[0, 0], orecv.at[d], o)

    def pair_of(d):
        return lax.rem(d // per_slice // 2 + 1, n_t // 2), lax.rem(d, per_slice)

    def y_copy(d, far):
        m, c = pair_of(d)
        return pltpu.make_async_remote_copy(
            src_ref=zsend.at[d], dst_ref=zrecv.at[far, m, c],
            send_sem=ysend.at[d], recv_sem=yrecv.at[far, m, c],
            device_id=(g, e, order(2 * m if far else 1)), device_id_type=MESH,
        )

    def y_arrived(far, m, c):
        pltpu.make_async_remote_copy(
            src_ref=zsend.at[0], dst_ref=zrecv.at[far, m, c],
            send_sem=ysend.at[0], recv_sem=yrecv.at[far, m, c],
            device_id=(g, e, order(1)), device_id_type=MESH,
        ).wait_recv()
        return zrecv[far, m, c].astype(jnp.float32)

    def combined(d):
        for o in range(1, n_e):
            o_arrived(o, d)
        return jnp.dot(place[...], recvbuf[d], preferred_element_type=jnp.float32)

    def combine_and_send(d):
        total = combined(d)
        odd = lax.rem(d // per_slice, 2)

        @pl.when(odd == 0)
        def _():
            zsend[d] = total.astype(jnp.bfloat16)
            y_copy(d, 0).start()

        @pl.when(odd == 1)
        def _():
            zsend[d] = (total + y_arrived(0, *pair_of(d))).astype(jnp.bfloat16)
            y_copy(d, 1).start()

    def expert_out(d, _):
        slot = lax.rem(gate_units + d, ring) * 2
        for copy in down_copies(d):
            copy.wait()
        value = jnp.dot(hidden[:, 0:kr], wbuf[slot, :, 0:dc], preferred_element_type=jnp.float32)
        for k in range(1, parts):
            value += jnp.dot(
                hidden[:, k * kr:(k + 1) * kr],
                wbuf[slot + k // per_slot, :, k % per_slot * dc:(k % per_slot + 1) * dc],
                preferred_element_type=jnp.float32,
            )
        for c in range(dc // LANES):
            lanes = slice(c * LANES, (c + 1) * LANES)
            sendbuf[d, :, lanes] = (value[:, lanes] * wslot[...]).astype(jnp.bfloat16)
        for o in range(1, n_e):
            o_copy(o, d).start()
        recvbuf[d, own_rows, :] = sendbuf[d, own_rows, :]
        if gate_units + ring < units:
            start_unit(gate_units + d + ring)

        @pl.when(jnp.logical_and(d >= lag, d - lag < down_chunks - per_slice))
        def _():
            combine_and_send(d - lag)

        return 0

    lax.fori_loop(0, down_chunks, expert_out, 0)

    def late(d, _):
        combine_and_send(d)
        return 0

    lax.fori_loop(max(0, down_chunks - lag), down_chunks - per_slice, late, 0)
    results = []
    for c in range(per_slice):
        total = combined(down_chunks - per_slice + c)
        total += y_arrived(0, 0, c)
        for m in range(1, n_t // 2):
            total += y_arrived(1, m, c)
        outbuf[:, c * dc:(c + 1) * dc] = total.astype(jnp.bfloat16)
        done = pltpu.make_async_copy(
            outbuf.at[:, c * dc:(c + 1) * dc], out.at[:, c * dc:(c + 1) * dc], lsem.at[3 + pieces + c]
        )
        done.start()
        results.append(done)

    for o in range(1, n_e):
        m_copy(o).wait_send()

    for j in range(1, n_t):
        for p in range(pieces):
            z_copy(j, p).wait_send()

    def drain_blocks(s, _):
        for p in range(pieces):
            for o in range(1, n_e):
                p_copy(o, s, p).wait_send()
        return 0

    lax.fori_loop(0, n_t, drain_blocks, 0)

    def drain_rows(d, _):
        for o in range(1, n_e):
            o_copy(o, d).wait_send()
        return 0

    lax.fori_loop(0, down_chunks, drain_rows, 0)

    def drain_sums(d, _):
        y_copy(d, 0).wait_send()
        return 0

    lax.fori_loop(0, down_chunks - per_slice, drain_sums, 0)
    for done in results:
        done.wait()


def per_device(n_e, n_t, tokens, norm_gain, w_gate, w_up, w_down, expert_ids, gate_weights):
    rows, kr = tokens.shape
    width, hid = w_gate.shape
    cap = rows // 2
    slots = n_e * cap
    sc = min(1024, hid)
    dc = min(512, kr)
    pieces = 2
    assert n_t > 1 and n_t & (n_t - 1) == 0
    assert hid % kr == 0 and hid // kr <= 2 * (sc // dc)
    per_slice = kr // dc
    down_chunks = n_t * per_slice
    units = n_t * (hid // sc) + down_chunks
    spent = (
        6 * rows * width + 8 * slots * width + 2 * slots * kr + 10 * slots * hid
        + 18 * slots * LANES + 2 * rows * kr + MIB
    )
    ring = min(units, (63 * MIB + MIB // 2 - spent) // (4 * kr * sc))
    hbm = pl.BlockSpec(memory_space=pl.ANY)
    bf16, f32, i32, dma = jnp.bfloat16, jnp.float32, jnp.int32, pltpu.SemaphoreType.DMA
    return pl.pallas_call(
        functools.partial(kernel, n_e, n_t, cap, ring, 3, pieces, dc),
        out_shape=jax.ShapeDtypeStruct((rows, kr), bf16),
        in_specs=[hbm] * 7,
        out_specs=hbm,
        scratch_shapes=[
            pltpu.VMEM((2 * ring, kr, sc), bf16),
            pltpu.VMEM((n_t, pieces, rows, kr // pieces), bf16),
            pltpu.VMEM((1, width), f32),
            pltpu.VMEM((2, rows), i32),
            pltpu.VMEM((2, rows), f32),
            pltpu.VMEM((slots, rows), bf16),
            pltpu.VMEM((rows, slots), bf16),
            pltpu.VMEM((slots, LANES), f32),
            pltpu.VMEM((slots, LANES), f32),
            pltpu.VMEM((n_t, pieces, slots, kr // pieces), bf16),
            pltpu.VMEM((n_t, pieces, slots, kr // pieces), bf16),
            pltpu.VMEM((pieces, slots, kr // pieces), bf16),
            pltpu.VMEM((slots, LANES), f32),
            pltpu.VMEM((slots, LANES), f32),
            pltpu.VMEM((slots, hid), f32),
            pltpu.VMEM((slots, hid), f32),
            pltpu.VMEM((slots, hid), bf16),
            pltpu.VMEM((down_chunks, slots, dc), bf16),
            pltpu.VMEM((down_chunks, slots, dc), bf16),
            pltpu.VMEM((down_chunks, rows, dc), bf16),
            pltpu.VMEM((2, n_t // 2, per_slice, rows, dc), bf16),
            pltpu.VMEM((rows, kr), bf16),
            dma((2 * ring, sc // dc)),
            dma((3 + pieces + per_slice,)),
            dma((n_t, pieces)),
            dma((n_t, pieces)),
            dma((n_e, n_t, pieces)),
            dma((n_t, pieces, n_e)),
            dma((n_e,)),
            dma((n_e,)),
            dma((n_e, down_chunks)),
            dma((down_chunks, n_e)),
            dma((down_chunks,)),
            dma((2, n_t // 2, per_slice)),
        ],
        compiler_params=pltpu.CompilerParams(
            collective_id=0, has_side_effects=True, vmem_limit_bytes=67043328
        ),
    )(tokens, norm_gain.reshape(1, width), expert_ids.T, gate_weights.T, w_gate, w_up, w_down)


def solution(mesh):
    in_specs = (
        P(("groups", "expert"), "tensor"),
        P(),
        P(None, ("expert", "tensor")),
        P(None, ("expert", "tensor")),
        P(("expert", "tensor"), None),
        P(("groups", "expert"), None),
        P(("groups", "expert"), None),
    )
    out_specs = P(("groups", "expert"), "tensor")
    body = functools.partial(per_device, mesh.shape["expert"], mesh.shape["tensor"])
    return jax.shard_map(body, mesh=mesh, in_specs=in_specs, out_specs=out_specs, check_vma=False)
```

```python
import functools

import jax
import jax.numpy as jnp
from jax import lax
from jax.experimental import pallas as pl
from jax.experimental.pallas import tpu as pltpu
from jax.sharding import PartitionSpec as P

EXPERTS = 8
MIB = 1 << 20
MESH = pl.DeviceIdType.MESH
LANES = 128


def kernel(
    n_e, n_t, cap, ring, lag, pieces, dc,
    tokens, gain_in, ids_in, weights_in, w_gate, w_up, w_down,
    out,
    wbuf, blocks, gain, ids, weights, spread, place, wsend, wslot, sendpk, recvpk, packed, ssq, scale,
    acc_gate, acc_up, hidden,
    sendbuf, recvbuf, zsend, zrecv,
    wsem, lsem, rsem, zsem, psend, precv, msend, mrecv, osend, orecv, ysend, yrecv,
):
    g, e, t = lax.axis_index("groups"), lax.axis_index("expert"), lax.axis_index("tensor")
    rows, kr = tokens.shape
    width = w_gate.shape[0]
    hid = w_gate.shape[1]
    sc = wbuf.shape[2]
    slots = n_e * cap
    per_expert = n_e * n_t // EXPERTS
    nj = hid // sc
    gate_units = n_t * nj
    parts = hid // kr
    per_slot = sc // dc
    per_slice = kr // dc
    down_chunks = n_t * per_slice
    units = gate_units + down_chunks
    kp = kr // pieces

    def order(s):
        return jnp.bitwise_xor(t, s)

    def slice_of(k):
        return order(2 * lax.rem(k // 2 + 1, n_t // 2) + 1 - lax.rem(k, 2))

    def columns(start, size):
        return pl.ds(pl.multiple_of(start, size), size)

    def down_columns(d):
        return columns(slice_of(d // per_slice) * kr + (d % per_slice) * dc, dc)

    def gate_copies(u, q, j):
        slot = lax.rem(u, ring) * 2
        at = (columns(q * kr, kr), columns(j * sc, sc))
        return (
            pltpu.make_async_copy(w_gate.at[at], wbuf.at[slot], wsem.at[slot, 0]),
            pltpu.make_async_copy(w_up.at[at], wbuf.at[slot + 1], wsem.at[slot + 1, 0]),
        )

    def down_copies(d):
        slot = lax.rem(gate_units + d, ring) * 2
        return [
            pltpu.make_async_copy(
                w_down.at[k * kr:(k + 1) * kr, down_columns(d)],
                wbuf.at[slot + k // per_slot, :, k % per_slot * dc:(k % per_slot + 1) * dc],
                wsem.at[slot + k // per_slot, k % per_slot],
            )
            for k in range(parts)
        ]

    def start_unit(u):
        @pl.when(u < gate_units)
        def _():
            for copy in gate_copies(u, order(u // nj), u % nj):
                copy.start()

        @pl.when(jnp.logical_and(u >= gate_units, u < units))
        def _():
            for copy in down_copies(u - gate_units):
                copy.start()

    def block_copy(q, p, send_sem, to):
        return pltpu.make_async_remote_copy(
            src_ref=blocks.at[q, p], dst_ref=blocks.at[q, p],
            send_sem=send_sem, recv_sem=rsem.at[q, p], device_id=(g, e, to), device_id_type=MESH,
        )

    def z_copy(j, p):
        return block_copy(t, p, zsem.at[j, p], order(j))

    def z_relay(s, p):
        return block_copy(order(s), p, zsem.at[s + 1, p], order(1))

    def rows_copy(src, dst, send_sem, recv_sem, o):
        ej = lax.rem(e + o, n_e)
        return pltpu.make_async_remote_copy(
            src_ref=src.at[columns(ej * cap, cap)], dst_ref=dst.at[columns(e * cap, cap)],
            send_sem=send_sem, recv_sem=recv_sem.at[e], device_id=(g, ej, t), device_id_type=MESH,
        )

    def rows_arrived(src, dst, send_sem, recv_sem, o):
        ej = lax.rem(e + o, n_e)
        at = columns(ej * cap, cap)
        pltpu.make_async_remote_copy(
            src_ref=src.at[at], dst_ref=dst.at[at],
            send_sem=send_sem, recv_sem=recv_sem.at[ej], device_id=(g, ej, t), device_id_type=MESH,
        ).wait_recv()

    def p_copy(o, q, p):
        return rows_copy(sendpk.at[q, p], recvpk.at[q, p], psend.at[o, q, p], precv.at[q, p], o)

    def m_copy(o):
        return rows_copy(wsend, wslot, msend.at[o], mrecv, o)

    own_rows = columns(e * cap, cap)

    local = [
        pltpu.make_async_copy(tokens.at[:, p * kp:(p + 1) * kp], blocks.at[t, p], lsem.at[3 + p])
        for p in range(pieces)
    ] + [
        pltpu.make_async_copy(ids_in, ids, lsem.at[0]),
        pltpu.make_async_copy(weights_in, weights, lsem.at[1]),
        pltpu.make_async_copy(gain_in, gain, lsem.at[2]),
    ]
    for copy in local:
        copy.start()
    barrier = pltpu.get_barrier_semaphore()
    for o in range(1, n_e):
        pl.semaphore_signal(barrier, inc=1, device_id=(g, lax.rem(e + o, n_e), t), device_id_type=MESH)
    for o in range(1, n_t):
        pl.semaphore_signal(barrier, inc=1, device_id=(g, e, lax.rem(t + o, n_t)), device_id_type=MESH)

    def prefetch(u, _):
        start_unit(u)
        return 0

    early = min(ring, units, 4)
    lax.fori_loop(0, early, prefetch, 0)
    for p in range(pieces):
        local[p].wait()
    pl.semaphore_wait(barrier, n_e - 1 + n_t - 1)
    for p in range(pieces):
        z_copy(1, p).start()
    for j in range(2, n_t, 2):
        for p in range(pieces):
            z_copy(j, p).start()
    for copy in local[pieces:]:
        copy.wait()

    upper = (
        lax.broadcasted_iota(jnp.int32, (rows, rows), 0) < lax.broadcasted_iota(jnp.int32, (rows, rows), 1)
    ).astype(jnp.float32).astype(jnp.bfloat16)

    hits = []
    for ej in range(n_e):
        expert = (ej * n_t + t) // per_expert
        named = jnp.where(ids[0:1, :] == expert, 1.0, 0.0) + jnp.where(ids[1:2, :] == expert, 1.0, 0.0)
        rank = jnp.dot(
            jnp.broadcast_to(named, (8, rows)).astype(jnp.bfloat16), upper, preferred_element_type=jnp.float32
        )[0:1, :]
        slot = lax.broadcasted_iota(jnp.int32, (cap, rows), 0).astype(jnp.float32)
        hits.append(jnp.where(slot == rank, 1.0, 0.0) * named)
        spread[ej * cap:(ej + 1) * cap, :] = hits[ej].astype(jnp.bfloat16)

    def dispatch(q, p):
        picked = jnp.dot(spread[...], blocks[q, p], preferred_element_type=jnp.float32)
        sendpk[q, p] = picked.astype(jnp.bfloat16)
        for o in range(1, n_e):
            p_copy(o, q, p).start()
        recvpk[q, p, own_rows, :] = sendpk[q, p, own_rows, :]

    def take(s):
        q = order(s)
        for p in range(pieces):
            block_copy(q, p, zsem.at[1, 0], order(1)).wait_recv()

            @pl.when(lax.rem(s, 2) == 0)
            def _():
                z_relay(s, p).start()

            dispatch(q, p)

    def pack(q):
        for p in range(pieces):
            for o in range(1, n_e):
                rows_arrived(sendpk.at[q, p], recvpk.at[q, p], psend.at[0, 0, 0], precv.at[q, p], o)
            gain_q = gain[:, columns(q * kr + p * kp, kp)]
            for r in range(slots // 32):
                at = slice(r * 32, (r + 1) * 32)
                value = recvpk[q, p, at, :].astype(jnp.float32)
                square = value * value
                total = square[:, 0:LANES]
                for c in range(1, kp // LANES):
                    total += square[:, c * LANES:(c + 1) * LANES]
                ssq[at, :] += total
                packed[p, at, :] = (value * gain_q).astype(jnp.bfloat16)

    def contract(ref, inner):
        value = jnp.dot(packed[0], ref[0:kp, inner], preferred_element_type=jnp.float32)
        for p in range(1, pieces):
            value += jnp.dot(packed[p], ref[p * kp:(p + 1) * kp, inner], preferred_element_type=jnp.float32)
        return value

    def expert_in(s, first, last):
        q = order(s)
        pack(q)
        if last:
            mean = jnp.sum(ssq[...], axis=1, keepdims=True) / width
            scale[...] = jnp.broadcast_to(lax.rsqrt(mean + 1e-05), scale.shape)

        def one(j, _):
            u = s * nj + j
            slot = lax.rem(u, ring) * 2
            if not last:
                @pl.when(j == nj // 2)
                def _():
                    @pl.when(s + 2 < n_t)
                    def _():
                        take(s + 2)

            for copy in gate_copies(u, q, j):
                copy.wait()
            wide = min(512, sc)
            for n in range(sc // wide):
                inner = slice(n * wide, (n + 1) * wide)
                at = columns(j * sc + n * wide, wide)
                gate = contract(wbuf.at[slot], inner)
                if not first:
                    gate += acc_gate[:, at]
                up = contract(wbuf.at[slot + 1], inner)
                if not first:
                    up += acc_up[:, at]
                if last:
                    for c in range(wide // LANES):
                        lanes = slice(c * LANES, (c + 1) * LANES)
                        gated = gate[:, lanes] * scale[...]
                        value = gated / (1.0 + jnp.exp(-gated)) * (up[:, lanes] * scale[...])
                        hidden[:, columns(j * sc + n * wide + c * LANES, LANES)] = value.astype(jnp.bfloat16)
                else:
                    acc_gate[:, at] = gate
                    acc_up[:, at] = up
            start_unit(u + ring)
            return 0

        lax.fori_loop(0, nj, one, 0)

    for p in range(pieces):
        dispatch(t, p)
    lax.fori_loop(early, min(ring, units), prefetch, 0)
    for ej in range(n_e):
        expert = (ej * n_t + t) // per_expert
        weight = jnp.where(ids[0:1, :] == expert, weights[0:1, :], weights[1:2, :])
        at = slice(ej * cap, (ej + 1) * cap)
        wsend[at, :] = jnp.broadcast_to(jnp.sum(hits[ej] * weight, axis=1, keepdims=True), (cap, LANES))
        filled = jnp.concatenate([hits[ej], jnp.zeros((cap, LANES - rows), jnp.float32)], axis=1)
        place[:, at] = jnp.transpose(filled)[0:rows, :].astype(jnp.bfloat16)
    wslot[own_rows, :] = wsend[own_rows, :]
    ssq[...] = jnp.zeros_like(ssq)
    take(jnp.int32(1))
    expert_in(jnp.int32(0), True, False)

    def middle(s, _):
        expert_in(s, False, False)
        return 0

    lax.fori_loop(1, n_t - 1, middle, 0)
    for o in range(1, n_e):
        m_copy(o).start()
    expert_in(jnp.int32(n_t - 1), False, True)

    for o in range(1, n_e):
        rows_arrived(wsend, wslot, msend.at[0], mrecv, o)

    def o_copy(o, d):
        return rows_copy(sendbuf.at[d], recvbuf.at[d], osend.at[o, d], orecv.at[d], o)

    def o_arrived(o, d):
        rows_arrived(sendbuf.at[d], recvbuf.at[d], osend.at[0, 0], orecv.at[d], o)

    def pair_of(d):
        return lax.rem(d // per_slice // 2 + 1, n_t // 2), lax.rem(d, per_slice)

    def y_copy(d, far):
        m, c = pair_of(d)
        return pltpu.make_async_remote_copy(
            src_ref=zsend.at[d], dst_ref=zrecv.at[far, m, c],
            send_sem=ysend.at[d], recv_sem=yrecv.at[far, m, c],
            device_id=(g, e, order(2 * m if far else 1)), device_id_type=MESH,
        )

    def y_arrived(far, m, c):
        pltpu.make_async_remote_copy(
            src_ref=zsend.at[0], dst_ref=zrecv.at[far, m, c],
            send_sem=ysend.at[0], recv_sem=yrecv.at[far, m, c],
            device_id=(g, e, order(1)), device_id_type=MESH,
        ).wait_recv()
        return zrecv[far, m, c].astype(jnp.float32)

    def combined(d):
        for o in range(1, n_e):
            o_arrived(o, d)
        return jnp.dot(place[...], recvbuf[d], preferred_element_type=jnp.float32)

    def combine_and_send(d):
        total = combined(d)
        odd = lax.rem(d // per_slice, 2)

        @pl.when(odd == 0)
        def _():
            zsend[d] = total.astype(jnp.bfloat16)
            y_copy(d, 0).start()

        @pl.when(odd == 1)
        def _():
            zsend[d] = (total + y_arrived(0, *pair_of(d))).astype(jnp.bfloat16)
            y_copy(d, 1).start()

    def expert_out(d, _):
        slot = lax.rem(gate_units + d, ring) * 2
        for copy in down_copies(d):
            copy.wait()
        value = jnp.dot(hidden[:, 0:kr], wbuf[slot, :, 0:dc], preferred_element_type=jnp.float32)
        for k in range(1, parts):
            value += jnp.dot(
                hidden[:, k * kr:(k + 1) * kr],
                wbuf[slot + k // per_slot, :, k % per_slot * dc:(k % per_slot + 1) * dc],
                preferred_element_type=jnp.float32,
            )
        for c in range(dc // LANES):
            lanes = slice(c * LANES, (c + 1) * LANES)
            sendbuf[d, :, lanes] = (value[:, lanes] * wslot[...]).astype(jnp.bfloat16)
        for o in range(1, n_e):
            o_copy(o, d).start()
        recvbuf[d, own_rows, :] = sendbuf[d, own_rows, :]
        if gate_units + ring < units:
            start_unit(gate_units + d + ring)

        @pl.when(jnp.logical_and(d >= lag, d - lag < down_chunks - per_slice))
        def _():
            combine_and_send(d - lag)

        return 0

    lax.fori_loop(0, down_chunks, expert_out, 0)

    def late(d, _):
        combine_and_send(d)
        return 0

    lax.fori_loop(max(0, down_chunks - lag), down_chunks - per_slice, late, 0)
    for c in range(per_slice):
        total = combined(down_chunks - per_slice + c)
        total += y_arrived(0, 0, c)
        for m in range(1, n_t // 2):
            total += y_arrived(1, m, c)
        out[:, c * dc:(c + 1) * dc] = total.astype(jnp.bfloat16)

    for o in range(1, n_e):
        m_copy(o).wait_send()

    for j in range(1, n_t):
        for p in range(pieces):
            z_copy(j, p).wait_send()

    def drain_blocks(s, _):
        for p in range(pieces):
            for o in range(1, n_e):
                p_copy(o, s, p).wait_send()
        return 0

    lax.fori_loop(0, n_t, drain_blocks, 0)

    def drain_rows(d, _):
        for o in range(1, n_e):
            o_copy(o, d).wait_send()
        return 0

    lax.fori_loop(0, down_chunks, drain_rows, 0)

    def drain_sums(d, _):
        y_copy(d, 0).wait_send()
        return 0

    lax.fori_loop(0, down_chunks - per_slice, drain_sums, 0)


def per_device(n_e, n_t, tokens, norm_gain, w_gate, w_up, w_down, expert_ids, gate_weights):
    rows, kr = tokens.shape
    width, hid = w_gate.shape
    cap = rows // 2
    slots = n_e * cap
    sc = min(1024, hid)
    dc = min(512, kr)
    pieces = 2
    assert n_t > 1 and n_t & (n_t - 1) == 0
    assert hid % kr == 0 and hid // kr <= 2 * (sc // dc)
    per_slice = kr // dc
    down_chunks = n_t * per_slice
    units = n_t * (hid // sc) + down_chunks
    out_bytes = max(2 * rows * kr, MIB // 4)
    spent = (
        6 * rows * width + 8 * slots * width + 2 * slots * kr + 10 * slots * hid
        + 18 * slots * LANES + 2 * rows * kr + MIB
    )
    ring = min(units, (63 * MIB + MIB // 2 - spent) // (4 * kr * sc))
    hbm = pl.BlockSpec(memory_space=pl.ANY)
    bf16, f32, i32, dma = jnp.bfloat16, jnp.float32, jnp.int32, pltpu.SemaphoreType.DMA
    return pl.pallas_call(
        functools.partial(kernel, n_e, n_t, cap, ring, 2, pieces, dc),
        out_shape=pltpu.VMEM((rows, kr), bf16),
        in_specs=[hbm] * 7,
        out_specs=pl.BlockSpec(memory_space=pltpu.VMEM),
        scratch_shapes=[
            pltpu.VMEM((2 * ring, kr, sc), bf16),
            pltpu.VMEM((n_t, pieces, rows, kr // pieces), bf16),
            pltpu.VMEM((1, width), f32),
            pltpu.VMEM((2, rows), i32),
            pltpu.VMEM((2, rows), f32),
            pltpu.VMEM((slots, rows), bf16),
            pltpu.VMEM((rows, slots), bf16),
            pltpu.VMEM((slots, LANES), f32),
            pltpu.VMEM((slots, LANES), f32),
            pltpu.VMEM((n_t, pieces, slots, kr // pieces), bf16),
            pltpu.VMEM((n_t, pieces, slots, kr // pieces), bf16),
            pltpu.VMEM((pieces, slots, kr // pieces), bf16),
            pltpu.VMEM((slots, LANES), f32),
            pltpu.VMEM((slots, LANES), f32),
            pltpu.VMEM((slots, hid), f32),
            pltpu.VMEM((slots, hid), f32),
            pltpu.VMEM((slots, hid), bf16),
            pltpu.VMEM((down_chunks, slots, dc), bf16),
            pltpu.VMEM((down_chunks, slots, dc), bf16),
            pltpu.VMEM((down_chunks, rows, dc), bf16),
            pltpu.VMEM((2, n_t // 2, per_slice, rows, dc), bf16),
            dma((2 * ring, sc // dc)),
            dma((3 + pieces,)),
            dma((n_t, pieces)),
            dma((n_t, pieces)),
            dma((n_e, n_t, pieces)),
            dma((n_t, pieces, n_e)),
            dma((n_e,)),
            dma((n_e,)),
            dma((n_e, down_chunks)),
            dma((down_chunks, n_e)),
            dma((down_chunks,)),
            dma((2, n_t // 2, per_slice)),
        ],
        compiler_params=pltpu.CompilerParams(
            collective_id=0, has_side_effects=True, vmem_limit_bytes=67043328 - 2 * out_bytes
        ),
    )(tokens, norm_gain.reshape(1, width), expert_ids.T, gate_weights.T, w_gate, w_up, w_down)


def solution(mesh):
    in_specs = (
        P(("groups", "expert"), "tensor"),
        P(),
        P(None, ("expert", "tensor")),
        P(None, ("expert", "tensor")),
        P(("expert", "tensor"), None),
        P(("groups", "expert"), None),
        P(("groups", "expert"), None),
    )
    out_specs = P(("groups", "expert"), "tensor")
    body = functools.partial(per_device, mesh.shape["expert"], mesh.shape["tensor"])
    return jax.shard_map(body, mesh=mesh, in_specs=in_specs, out_specs=out_specs, check_vma=False)
```

```python
import functools

import jax
import jax.numpy as jnp
from jax import lax
from jax.experimental import pallas as pl
from jax.experimental.pallas import tpu as pltpu
from jax.sharding import PartitionSpec as P

EXPERTS = 8
MIB = 1 << 20
MESH = pl.DeviceIdType.MESH
LANES = 128


def kernel(
    n_e, n_t, cap, ring, lag, pieces, dc,
    tokens, gain_in, ids_in, weights_in, w_gate, w_up, w_down,
    out,
    wbuf, blocks, gain, ids, weights, spread, place, wsend, wslot, sendpk, recvpk, packed, ssq, scale,
    acc_gate, acc_up, hidden,
    sendbuf, recvbuf, zsend, zrecv,
    wsem, lsem, rsem, zsem, psend, precv, msend, mrecv, osend, orecv, ysend, yrecv,
):
    g, e, t = lax.axis_index("groups"), lax.axis_index("expert"), lax.axis_index("tensor")
    rows, kr = tokens.shape
    width = w_gate.shape[0]
    hid = w_gate.shape[1]
    sc = wbuf.shape[2]
    slots = n_e * cap
    per_expert = n_e * n_t // EXPERTS
    nj = hid // sc
    gate_units = n_t * nj
    parts = hid // kr
    per_slot = sc // dc
    per_slice = kr // dc
    down_chunks = n_t * per_slice
    units = gate_units + down_chunks
    kp = kr // pieces

    def order(s):
        return jnp.bitwise_xor(t, s)

    def slice_of(k):
        return order(2 * lax.rem(k // 2 + 1, n_t // 2) + 1 - lax.rem(k, 2))

    def columns(start, size):
        return pl.ds(pl.multiple_of(start, size), size)

    def down_columns(d):
        return columns(slice_of(d // per_slice) * kr + (d % per_slice) * dc, dc)

    def gate_copies(u, q, j):
        slot = lax.rem(u, ring) * 2
        at = (columns(q * kr, kr), columns(j * sc, sc))
        return (
            pltpu.make_async_copy(w_gate.at[at], wbuf.at[slot], wsem.at[slot, 0]),
            pltpu.make_async_copy(w_up.at[at], wbuf.at[slot + 1], wsem.at[slot + 1, 0]),
        )

    def down_copies(d):
        slot = lax.rem(gate_units + d, ring) * 2
        return [
            pltpu.make_async_copy(
                w_down.at[k * kr:(k + 1) * kr, down_columns(d)],
                wbuf.at[slot + k // per_slot, :, k % per_slot * dc:(k % per_slot + 1) * dc],
                wsem.at[slot + k // per_slot, k % per_slot],
            )
            for k in range(parts)
        ]

    def start_unit(u):
        @pl.when(u < gate_units)
        def _():
            for copy in gate_copies(u, order(u // nj), u % nj):
                copy.start()

        @pl.when(jnp.logical_and(u >= gate_units, u < units))
        def _():
            for copy in down_copies(u - gate_units):
                copy.start()

    def block_copy(q, p, send_sem, to):
        return pltpu.make_async_remote_copy(
            src_ref=blocks.at[q, p], dst_ref=blocks.at[q, p],
            send_sem=send_sem, recv_sem=rsem.at[q, p], device_id=(g, e, to), device_id_type=MESH,
        )

    def z_copy(j, p):
        return block_copy(t, p, zsem.at[j, p], order(j))

    def z_relay(s, p):
        return block_copy(order(s), p, zsem.at[s + 1, p], order(1))

    def rows_copy(src, dst, send_sem, recv_sem, o):
        ej = lax.rem(e + o, n_e)
        return pltpu.make_async_remote_copy(
            src_ref=src.at[columns(ej * cap, cap)], dst_ref=dst.at[columns(e * cap, cap)],
            send_sem=send_sem, recv_sem=recv_sem.at[e], device_id=(g, ej, t), device_id_type=MESH,
        )

    def rows_arrived(src, dst, send_sem, recv_sem, o):
        ej = lax.rem(e + o, n_e)
        at = columns(ej * cap, cap)
        pltpu.make_async_remote_copy(
            src_ref=src.at[at], dst_ref=dst.at[at],
            send_sem=send_sem, recv_sem=recv_sem.at[ej], device_id=(g, ej, t), device_id_type=MESH,
        ).wait_recv()

    def p_copy(o, q, p):
        return rows_copy(sendpk.at[q, p], recvpk.at[q, p], psend.at[o, q, p], precv.at[q, p], o)

    def m_copy(o):
        return rows_copy(wsend, wslot, msend.at[o], mrecv, o)

    own_rows = columns(e * cap, cap)

    local = [
        pltpu.make_async_copy(tokens.at[:, p * kp:(p + 1) * kp], blocks.at[t, p], lsem.at[3 + p])
        for p in range(pieces)
    ] + [
        pltpu.make_async_copy(ids_in, ids, lsem.at[0]),
        pltpu.make_async_copy(weights_in, weights, lsem.at[1]),
        pltpu.make_async_copy(gain_in, gain, lsem.at[2]),
    ]
    for copy in local:
        copy.start()
    barrier = pltpu.get_barrier_semaphore()
    for o in range(1, n_e):
        pl.semaphore_signal(barrier, inc=1, device_id=(g, lax.rem(e + o, n_e), t), device_id_type=MESH)
    for o in range(1, n_t):
        pl.semaphore_signal(barrier, inc=1, device_id=(g, e, lax.rem(t + o, n_t)), device_id_type=MESH)

    def prefetch(u, _):
        start_unit(u)
        return 0

    early = min(ring, units, 4)
    lax.fori_loop(0, early, prefetch, 0)
    for p in range(pieces):
        local[p].wait()
    pl.semaphore_wait(barrier, n_e - 1 + n_t - 1)
    for p in range(pieces):
        z_copy(1, p).start()
    for j in range(2, n_t, 2):
        for p in range(pieces):
            z_copy(j, p).start()
    for copy in local[pieces:]:
        copy.wait()

    upper = (
        lax.broadcasted_iota(jnp.int32, (rows, rows), 0) < lax.broadcasted_iota(jnp.int32, (rows, rows), 1)
    ).astype(jnp.float32).astype(jnp.bfloat16)

    hits = []
    for ej in range(n_e):
        expert = (ej * n_t + t) // per_expert
        named = jnp.where(ids[0:1, :] == expert, 1.0, 0.0) + jnp.where(ids[1:2, :] == expert, 1.0, 0.0)
        rank = jnp.dot(
            jnp.broadcast_to(named, (8, rows)).astype(jnp.bfloat16), upper, preferred_element_type=jnp.float32
        )[0:1, :]
        slot = lax.broadcasted_iota(jnp.int32, (cap, rows), 0).astype(jnp.float32)
        hits.append(jnp.where(slot == rank, 1.0, 0.0) * named)
        spread[ej * cap:(ej + 1) * cap, :] = hits[ej].astype(jnp.bfloat16)

    def dispatch(q, p):
        picked = jnp.dot(spread[...], blocks[q, p], preferred_element_type=jnp.float32)
        sendpk[q, p] = picked.astype(jnp.bfloat16)
        for o in range(1, n_e):
            p_copy(o, q, p).start()
        recvpk[q, p, own_rows, :] = sendpk[q, p, own_rows, :]

    def take(s):
        q = order(s)
        for p in range(pieces):
            block_copy(q, p, zsem.at[1, 0], order(1)).wait_recv()

            @pl.when(lax.rem(s, 2) == 0)
            def _():
                z_relay(s, p).start()

            dispatch(q, p)

    def pack(q):
        for p in range(pieces):
            for o in range(1, n_e):
                rows_arrived(sendpk.at[q, p], recvpk.at[q, p], psend.at[0, 0, 0], precv.at[q, p], o)
            gain_q = gain[:, columns(q * kr + p * kp, kp)]
            for r in range(slots // 32):
                at = slice(r * 32, (r + 1) * 32)
                value = recvpk[q, p, at, :].astype(jnp.float32)
                square = value * value
                total = square[:, 0:LANES]
                for c in range(1, kp // LANES):
                    total += square[:, c * LANES:(c + 1) * LANES]
                ssq[at, :] += total
                packed[p, at, :] = (value * gain_q).astype(jnp.bfloat16)

    def contract(ref, inner):
        value = jnp.dot(packed[0], ref[0:kp, inner], preferred_element_type=jnp.float32)
        for p in range(1, pieces):
            value += jnp.dot(packed[p], ref[p * kp:(p + 1) * kp, inner], preferred_element_type=jnp.float32)
        return value

    def expert_in(s, first, last):
        q = order(s)
        pack(q)
        if last:
            mean = jnp.sum(ssq[...], axis=1, keepdims=True) / width
            scale[...] = jnp.broadcast_to(lax.rsqrt(mean + 1e-05), scale.shape)

        def one(j, _):
            u = s * nj + j
            slot = lax.rem(u, ring) * 2
            if not last:
                @pl.when(j == nj // 2)
                def _():
                    @pl.when(s + 2 < n_t)
                    def _():
                        take(s + 2)

            for copy in gate_copies(u, q, j):
                copy.wait()
            wide = min(512, sc)
            for n in range(sc // wide):
                inner = slice(n * wide, (n + 1) * wide)
                at = columns(j * sc + n * wide, wide)
                gate = contract(wbuf.at[slot], inner)
                if not first:
                    gate += acc_gate[:, at]
                up = contract(wbuf.at[slot + 1], inner)
                if not first:
                    up += acc_up[:, at]
                if last:
                    for c in range(wide // LANES):
                        lanes = slice(c * LANES, (c + 1) * LANES)
                        gated = gate[:, lanes] * scale[...]
                        value = gated / (1.0 + jnp.exp(-gated)) * (up[:, lanes] * scale[...])
                        hidden[:, columns(j * sc + n * wide + c * LANES, LANES)] = value.astype(jnp.bfloat16)
                else:
                    acc_gate[:, at] = gate
                    acc_up[:, at] = up
            start_unit(u + ring)
            return 0

        lax.fori_loop(0, nj, one, 0)

    for p in range(pieces):
        dispatch(t, p)
    lax.fori_loop(early, min(ring, units), prefetch, 0)
    for ej in range(n_e):
        expert = (ej * n_t + t) // per_expert
        weight = jnp.where(ids[0:1, :] == expert, weights[0:1, :], weights[1:2, :])
        at = slice(ej * cap, (ej + 1) * cap)
        wsend[at, :] = jnp.broadcast_to(jnp.sum(hits[ej] * weight, axis=1, keepdims=True), (cap, LANES))
        filled = jnp.concatenate([hits[ej], jnp.zeros((cap, LANES - rows), jnp.float32)], axis=1)
        place[:, at] = jnp.transpose(filled)[0:rows, :].astype(jnp.bfloat16)
    wslot[own_rows, :] = wsend[own_rows, :]
    ssq[...] = jnp.zeros_like(ssq)
    take(jnp.int32(1))
    expert_in(jnp.int32(0), True, False)

    def middle(s, _):
        expert_in(s, False, False)
        return 0

    lax.fori_loop(1, n_t - 1, middle, 0)
    for o in range(1, n_e):
        m_copy(o).start()
    expert_in(jnp.int32(n_t - 1), False, True)

    for o in range(1, n_e):
        rows_arrived(wsend, wslot, msend.at[0], mrecv, o)

    def o_copy(o, d):
        return rows_copy(sendbuf.at[d], recvbuf.at[d], osend.at[o, d], orecv.at[d], o)

    def o_arrived(o, d):
        rows_arrived(sendbuf.at[d], recvbuf.at[d], osend.at[0, 0], orecv.at[d], o)

    def pair_of(d):
        return lax.rem(d // per_slice // 2 + 1, n_t // 2), lax.rem(d, per_slice)

    def y_copy(d, far):
        m, c = pair_of(d)
        return pltpu.make_async_remote_copy(
            src_ref=zsend.at[d], dst_ref=zrecv.at[far, m, c],
            send_sem=ysend.at[d], recv_sem=yrecv.at[far, m, c],
            device_id=(g, e, order(2 * m if far else 1)), device_id_type=MESH,
        )

    def y_arrived(far, m, c):
        pltpu.make_async_remote_copy(
            src_ref=zsend.at[0], dst_ref=zrecv.at[far, m, c],
            send_sem=ysend.at[0], recv_sem=yrecv.at[far, m, c],
            device_id=(g, e, order(1)), device_id_type=MESH,
        ).wait_recv()
        return zrecv[far, m, c].astype(jnp.float32)

    def combined(d):
        for o in range(1, n_e):
            o_arrived(o, d)
        return jnp.dot(place[...], recvbuf[d], preferred_element_type=jnp.float32)

    def combine_and_send(d):
        total = combined(d)
        odd = lax.rem(d // per_slice, 2)

        @pl.when(odd == 0)
        def _():
            zsend[d] = total.astype(jnp.bfloat16)
            y_copy(d, 0).start()

        @pl.when(odd == 1)
        def _():
            zsend[d] = (total + y_arrived(0, *pair_of(d))).astype(jnp.bfloat16)
            y_copy(d, 1).start()

    def expert_out(d, _):
        slot = lax.rem(gate_units + d, ring) * 2
        for copy in down_copies(d):
            copy.wait()
        value = jnp.dot(hidden[:, 0:kr], wbuf[slot, :, 0:dc], preferred_element_type=jnp.float32)
        for k in range(1, parts):
            value += jnp.dot(
                hidden[:, k * kr:(k + 1) * kr],
                wbuf[slot + k // per_slot, :, k % per_slot * dc:(k % per_slot + 1) * dc],
                preferred_element_type=jnp.float32,
            )
        for c in range(dc // LANES):
            lanes = slice(c * LANES, (c + 1) * LANES)
            sendbuf[d, :, lanes] = (value[:, lanes] * wslot[...]).astype(jnp.bfloat16)
        for o in range(1, n_e):
            o_copy(o, d).start()
        recvbuf[d, own_rows, :] = sendbuf[d, own_rows, :]
        if gate_units + ring < units:
            start_unit(gate_units + d + ring)

        @pl.when(jnp.logical_and(d >= lag, d - lag < down_chunks - per_slice))
        def _():
            combine_and_send(d - lag)

        return 0

    lax.fori_loop(0, down_chunks, expert_out, 0)

    def late(d, _):
        combine_and_send(d)
        return 0

    lax.fori_loop(max(0, down_chunks - lag), down_chunks - per_slice, late, 0)
    for o in range(1, n_e):
        m_copy(o).wait_send()

    for j in range(1, n_t):
        for p in range(pieces):
            z_copy(j, p).wait_send()

    def drain_blocks(s, _):
        for p in range(pieces):
            for o in range(1, n_e):
                p_copy(o, s, p).wait_send()
        return 0

    lax.fori_loop(0, n_t, drain_blocks, 0)

    for c in range(per_slice):
        if c == per_slice - 1:
            def drain_rows(d, _):
                for o in range(1, n_e):
                    o_copy(o, d).wait_send()
                return 0

            lax.fori_loop(0, down_chunks, drain_rows, 0)

            def drain_sums(d, _):
                y_copy(d, 0).wait_send()
                return 0

            lax.fori_loop(0, down_chunks - per_slice, drain_sums, 0)

        total = combined(down_chunks - per_slice + c)
        total += y_arrived(0, 0, c)
        for m in range(1, n_t // 2):
            total += y_arrived(1, m, c)
        out[:, c * dc:(c + 1) * dc] = total.astype(jnp.bfloat16)


def per_device(n_e, n_t, tokens, norm_gain, w_gate, w_up, w_down, expert_ids, gate_weights):
    rows, kr = tokens.shape
    width, hid = w_gate.shape
    cap = rows // 2
    slots = n_e * cap
    sc = min(1024, hid)
    dc = min(512, kr)
    pieces = 2
    assert n_t > 1 and n_t & (n_t - 1) == 0
    assert hid % kr == 0 and hid // kr <= 2 * (sc // dc)
    per_slice = kr // dc
    down_chunks = n_t * per_slice
    units = n_t * (hid // sc) + down_chunks
    out_bytes = max(2 * rows * kr, MIB // 4)
    spent = (
        6 * rows * width + 8 * slots * width + 2 * slots * kr + 10 * slots * hid
        + 18 * slots * LANES + 2 * rows * kr + MIB
    )
    ring = min(units, (63 * MIB + MIB // 2 - spent) // (4 * kr * sc))
    hbm = pl.BlockSpec(memory_space=pl.ANY)
    bf16, f32, i32, dma = jnp.bfloat16, jnp.float32, jnp.int32, pltpu.SemaphoreType.DMA
    return pl.pallas_call(
        functools.partial(kernel, n_e, n_t, cap, ring, 2, pieces, dc),
        out_shape=pltpu.VMEM((rows, kr), bf16),
        in_specs=[hbm] * 7,
        out_specs=pl.BlockSpec(memory_space=pltpu.VMEM),
        scratch_shapes=[
            pltpu.VMEM((2 * ring, kr, sc), bf16),
            pltpu.VMEM((n_t, pieces, rows, kr // pieces), bf16),
            pltpu.VMEM((1, width), f32),
            pltpu.VMEM((2, rows), i32),
            pltpu.VMEM((2, rows), f32),
            pltpu.VMEM((slots, rows), bf16),
            pltpu.VMEM((rows, slots), bf16),
            pltpu.VMEM((slots, LANES), f32),
            pltpu.VMEM((slots, LANES), f32),
            pltpu.VMEM((n_t, pieces, slots, kr // pieces), bf16),
            pltpu.VMEM((n_t, pieces, slots, kr // pieces), bf16),
            pltpu.VMEM((pieces, slots, kr // pieces), bf16),
            pltpu.VMEM((slots, LANES), f32),
            pltpu.VMEM((slots, LANES), f32),
            pltpu.VMEM((slots, hid), f32),
            pltpu.VMEM((slots, hid), f32),
            pltpu.VMEM((slots, hid), bf16),
            pltpu.VMEM((down_chunks, slots, dc), bf16),
            pltpu.VMEM((down_chunks, slots, dc), bf16),
            pltpu.VMEM((down_chunks, rows, dc), bf16),
            pltpu.VMEM((2, n_t // 2, per_slice, rows, dc), bf16),
            dma((2 * ring, sc // dc)),
            dma((3 + pieces,)),
            dma((n_t, pieces)),
            dma((n_t, pieces)),
            dma((n_e, n_t, pieces)),
            dma((n_t, pieces, n_e)),
            dma((n_e,)),
            dma((n_e,)),
            dma((n_e, down_chunks)),
            dma((down_chunks, n_e)),
            dma((down_chunks,)),
            dma((2, n_t // 2, per_slice)),
        ],
        compiler_params=pltpu.CompilerParams(
            collective_id=0, has_side_effects=True, vmem_limit_bytes=67043328 - 2 * out_bytes
        ),
    )(tokens, norm_gain.reshape(1, width), expert_ids.T, gate_weights.T, w_gate, w_up, w_down)


def solution(mesh):
    in_specs = (
        P(("groups", "expert"), "tensor"),
        P(),
        P(None, ("expert", "tensor")),
        P(None, ("expert", "tensor")),
        P(("expert", "tensor"), None),
        P(("groups", "expert"), None),
        P(("groups", "expert"), None),
    )
    out_specs = P(("groups", "expert"), "tensor")
    body = functools.partial(per_device, mesh.shape["expert"], mesh.shape["tensor"])
    return jax.shard_map(body, mesh=mesh, in_specs=in_specs, out_specs=out_specs, check_vma=False)
```
